256 devices in a mesh: dp: 16 (over y_hi, z), mp: 16 (over x, y_lo, core).
Axes of the slice: x: 4, y: 4 (y_hi: 2, y_lo: 2; y = y_hi * 2 + y_lo), z: 8, core: 2. Of those that a mesh axis runs over, the one named last changes fastest.
Arguments:
- query_inputs: bfloat16 [512, 28672], P(None, 'mp'), may hold values from -0.09375 to 0.09375
- query_grads: bfloat16 [512, 8192], P(None, 'mp'), may hold values from -6 to 6
- basis_inputs: bfloat16 [28672, 28672], P('mp', 'dp'), may hold values from -0.03125 to 0.03125
- basis_grads: bfloat16 [8192, 8192], P('mp', 'dp'), may hold values from -0.0625 to 0.0625
- eig_inputs: float32 [28672], P('dp'), may hold values from 0.25 to 4
- eig_grads: float32 [8192], P('dp'), may hold values from 0.25 to 4
- train_inputs: bfloat16 [12288, 28672], P('dp', 'mp'), may hold values from -0.03540039 to 0.03540039
- train_grads: bfloat16 [12288, 8192], P('dp', 'mp'), may hold values from -0.06591797 to 0.06591797
Outputs:
- scores: float32 [16, 96], P('mp', 'dp')
The draws below stay inside these ranges and needn't reach their ends.
All inputs are finite; a program needn't handle non-finite values.
Results may differ from the reference program's by a relative error of at most 0.0054.
Values may be sent and summed in bfloat16 or wider, within the bound.
No kernel may reach another device: no remote copies, remote signals or barrier semaphores. Data moves between devices by JAX's collectives and lax.ppermute only.
A program may use at most 64 MiB of HBM per device.

```python
import math
import jax
import jax.numpy as jnp
from jax import lax

FA = 28672
FS = 8192
LEN = 128
QLEN = 32
NQ = 16
QT = 512
NSEQ = 96
TRAIN_TOK = 12288


def block_scale(own_key, dims, pieces, smallest, high):
    def one(position, shards_of):
        draws = jax.random.uniform(jax.random.fold_in(jax.random.fold_in(own_key, 6), position), (shards_of,), jnp.float32, smallest / len(pieces), high / len(pieces))
        return jnp.repeat(jnp.exp(draws), dims[position] // shards_of).reshape((-1,) + (1,) * (len(dims) - position - 1))

    gain = one(*pieces[0])
    for cut in pieces[1:]:
        gain = gain * one(*cut)
    return gain


def gaussian(own_key, shape, scale, most, split=(), held_as=jnp.bfloat16):
    drawn = scale * jax.random.normal(own_key, shape, jnp.float32)
    if split:
        drawn = drawn * block_scale(own_key, shape, split, -0.22, 0.18)
    return jnp.clip(drawn, -most, most).astype(held_as)


def setup_inputs(seed: int = 0) -> dict:
    keys = jax.random.split(jax.random.key(seed), 9)
    return {
        "query_inputs": gaussian(keys[0], (QT, FA), ((QLEN * LEN) ** -0.5), 0.09375, ((1, 16),)),
        "query_grads": gaussian(keys[1], (QT, FS), 1.0, 6.0, ((1, 16),)),
        "basis_inputs": gaussian(keys[2], (FA, FA), FA ** -0.5, 0.03125, ((0, 16), (1, 16))),
        "basis_grads": gaussian(keys[3], (FS, FS), FS ** -0.5, 0.0625, ((0, 16), (1, 16))),
        "eig_inputs": jnp.clip(jnp.exp(math.log(4.0) - 2.7725887 * jax.random.uniform(keys[4], (FA,), jnp.float32) ** block_scale(keys[4], (FA,), ((0, 16),), -0.2, 0.2)), 0.25, 4.0),
        "eig_grads": jnp.clip(jnp.exp(math.log(4.0) - 2.7725887 * jax.random.uniform(keys[5], (FS,), jnp.float32) ** block_scale(keys[5], (FS,), ((0, 16),), -0.2, 0.2)), 0.25, 4.0),
        "train_inputs": gaussian(keys[6], (TRAIN_TOK, FA), (FA ** -0.5), 0.03540039, ((0, 16), (1, 16))),
        "train_grads": gaussian(keys[7], (TRAIN_TOK, FS), (FS ** -0.5), 0.06591797, ((0, 16), (1, 16))),
    }


def precondition(factors, basis, eigen):
    rotated = jnp.dot(factors, basis, preferred_element_type=jnp.float32)
    scaled = (rotated / eigen[None, :]).astype(jnp.bfloat16)
    return jnp.dot(scaled, basis.T, preferred_element_type=jnp.float32).astype(jnp.bfloat16)


def reference(query_inputs, query_grads, basis_inputs, basis_grads, eig_inputs, eig_grads, train_inputs, train_grads):
    pre_in = precondition(query_inputs, basis_inputs, eig_inputs)
    pre_out = precondition(query_grads, basis_grads, eig_grads)
    seq_inputs = train_inputs.reshape(NSEQ, LEN, FA)
    seq_grads = train_grads.reshape(NSEQ, LEN, FS)

    def one_sequence(pair):
        seq_in, seq_out = pair
        inner_in = jnp.dot(pre_in, seq_in.T, preferred_element_type=jnp.float32)
        inner_out = jnp.dot(pre_out, seq_out.T, preferred_element_type=jnp.float32)
        products = inner_in * inner_out
        return jnp.sum(products.reshape(NQ, QLEN, LEN), axis=(1, 2))

    per_sequence = lax.map(one_sequence, (seq_inputs, seq_grads))
    return per_sequence.T
```

```python
import jax
import jax.numpy as jnp
from jax import lax
from jax.sharding import PartitionSpec as P

LEN = 128
QLEN = 32
CHUNKS = 2
F32, BF16 = jnp.float32, jnp.bfloat16


X, YL, C, YH, Z = 4, 2, 2, 2, 8
MP = [(x, y, c) for x in range(X) for y in range(YL) for c in range(C)]
DP = [(y, z) for y in range(YH) for z in range(Z)]


def mp_at(x, y, c):
    return (x % X) * 4 + (y % YL) * 2 + c % C


def dp_at(y, z):
    return (y % YH) * Z + z % Z


def move_x(v, by):
    return lax.ppermute(v, "mp", [(mp_at(x, y, c), mp_at(x + by, y, c)) for x, y, c in MP])


def swap_yl(v):
    return lax.ppermute(v, "mp", [(mp_at(x, y, c), mp_at(x, y + 1, c)) for x, y, c in MP])


def swap_core(v):
    return lax.ppermute(v, "mp", [(mp_at(x, y, c), mp_at(x, y, c + 1)) for x, y, c in MP])


def move_z(v, by):
    return lax.ppermute(v, "dp", [(dp_at(y, z), dp_at(y, z + by)) for y, z in DP])


def swap_yh(v):
    return lax.ppermute(v, "dp", [(dp_at(y, z), dp_at(y + 1, z)) for y, z in DP])


def at(v, i):
    return lax.dynamic_index_in_dim(v, i, 0, keepdims=False)


def half_added(v, half, extra):
    parts = [v[0], v[1]]
    parts[half] = parts[half] + extra
    return jnp.stack(parts)


def sum_over_x(seg):
    far = seg(2)
    up, down = move_x(far[0], 1), move_x(far[1], -1)
    from_below = move_x(half_added(seg(1), 0, up), 1)
    from_above = move_x(half_added(seg(3), 1, down), -1)
    return seg(0) + from_below + from_above


def split(v):
    high = lax.reduce_precision(v, 8, 7)
    return high.astype(BF16), (v - high).astype(BF16)


def per_device(
    query_inputs,
    query_grads,
    basis_inputs,
    basis_grads,
    eig_inputs,
    eig_grads,
    train_inputs,
    train_grads,
):
    tokens, feat_in = query_inputs.shape
    feat_out = query_grads.shape[1]
    cols_in, cols_out = basis_inputs.shape[1], basis_grads.shape[1]
    train_count = train_inputs.shape[0]
    rows = tokens // (CHUNKS * len(MP))
    m, d = lax.axis_index("mp"), lax.axis_index("dp")
    my_x, my_yl, my_c = m // 4, (m // 2) % 2, m % 2
    my_yh, my_z = d // Z, d % Z
    eig = jnp.concatenate([eig_inputs, eig_grads])[None, :]
    q_in = query_inputs.reshape(X, YL, C, CHUNKS, rows, feat_in)
    q_out = query_grads.reshape(X, YL, C, CHUNKS, rows, feat_out)

    def rotate(k, core):
        def of(q, basis):
            mine = lax.dynamic_index_in_dim(q[:, :, :, k], core, 2, keepdims=False)
            return jnp.dot(mine.reshape(-1, q.shape[-1]), basis, preferred_element_type=F32)

        both = jnp.concatenate([of(q_in, basis_inputs), of(q_out, basis_grads)], axis=1)
        return both.reshape(X, YL, rows, cols_in + cols_out)

    def rotated_and_scaled(k):
        other = swap_core(rotate(k, 1 - my_c))
        mine = rotate(k, my_c) + other
        total = sum_over_x(lambda r: at(mine, (my_x + r) % X))
        final = at(total, my_yl) + swap_yl(at(total, 1 - my_yl))
        return (final / eig).astype(BF16)

    def everyones(own):
        pair = jnp.stack([own, swap_yl(own)])
        below, above = move_x(pair, 1), move_x(pair, -1)
        far = jnp.stack([move_x(below[0], 1), move_x(above[1], -1)])
        mine = jnp.stack([pair, above, far, below])
        return mine, swap_core(mine)

    def back(own):
        mine, other = everyones(own)
        ins, outs = [], []
        for part in (mine, other):
            flat = part.reshape(-1, cols_in + cols_out)
            ins.append(jnp.einsum("qc,fc->qf", flat[:, :cols_in], basis_inputs, preferred_element_type=F32))
            outs.append(jnp.einsum("qc,fc->qf", flat[:, cols_in:], basis_grads, preferred_element_type=F32))
        v_in = jnp.stack(ins).reshape(Z, YH, rows, feat_in)
        v_out = jnp.stack(outs).reshape(Z, YH, rows, feat_out)
        return v_in, v_out

    def pack(v_in, v_out):
        high, low = split(v_out)
        return jnp.concatenate([v_in.astype(BF16), high, low], axis=-1)

    def unpack(v):
        v_in, high, low = jnp.split(v, [feat_in, feat_in + feat_out], axis=-1)
        return v_in.astype(F32), high.astype(F32) + low.astype(F32)

    def summed_over_dp(v_in, v_out):
        def chain(half, by):
            def seg(r):
                i = (my_z + by * r) % Z
                return at(v_in, i), at(v_out, i)

            s_in, s_out = seg(4)
            r_in, r_out = unpack(move_z(pack(s_in[half], s_out[half]), by))
            s_in, s_out = seg(3)
            got = move_z(pack(half_added(s_in, half, r_in), half_added(s_out, half, r_out)), by)
            for r in (2, 1):
                s_in, s_out = seg(r)
                r_in, r_out = unpack(got)
                got = move_z(pack(s_in + r_in, s_out + r_out), by)
            return unpack(got)

        up_in, up_out = chain(0, 1)
        down_in, down_out = chain(1, -1)
        total = jnp.concatenate(
            [at(v_in, my_z) + up_in + down_in, at(v_out, my_z) + up_out + down_out], axis=-1
        )
        return (at(total, my_yh) + swap_yh(at(total, 1 - my_yh))).astype(BF16)

    def gathered_over_dp(own):
        other = swap_yh(own)
        pair = jnp.where(my_yh == 0, jnp.stack([own, other]), jnp.stack([other, own]))
        whole = jnp.zeros((Z, *pair.shape), BF16)

        def put(whole, v, r):
            return lax.dynamic_update_index_in_dim(whole, v, (my_z + r) % Z, 0)

        whole = put(whole, pair, 0)
        up, down = pair, pair
        for r in (1, 2, 3):
            up, down = move_z(up, 1), move_z(down, -1)
            whole = put(put(whole, up, -r), down, r)
        return put(whole, jnp.stack([move_z(up[0], 1), move_z(down[1], -1)]), 4)

    def scores_of(directions):
        parts = directions.reshape(C, X * YL * rows, feat_in + feat_out)

        def inner(core):
            v_in = jnp.einsum("qf,tf->qt", parts[core, :, :feat_in], train_inputs, preferred_element_type=F32)
            v_out = jnp.einsum("qf,tf->qt", parts[core, :, feat_in:], train_grads, preferred_element_type=F32)
            return jnp.concatenate([v_in, v_out], axis=1).reshape(X, YL, rows, 2 * train_count)

        other = swap_core(inner(1))
        mine = inner(0) + other
        total = sum_over_x(lambda r: mine[r])
        final = total[0] + swap_yl(total[1])
        products = final[:, :train_count] * final[:, train_count:]
        return jnp.sum(products.reshape(rows, train_count // LEN, LEN), axis=(0, 2))

    result = 0.0
    for k in range(CHUNKS):
        own = rotated_and_scaled(k)
        own = summed_over_dp(*back(own))
        result = result + scores_of(gathered_over_dp(own))
    return result[None, :]


def solution(mesh):
    return jax.shard_map(
        per_device,
        mesh=mesh,
        in_specs=(
            P(None, "mp"),
            P(None, "mp"),
            P("mp", "dp"),
            P("mp", "dp"),
            P("dp"),
            P("dp"),
            P("dp", "mp"),
            P("dp", "mp"),
        ),
        out_specs=P("mp", "dp"),
        check_vma=False,
    )
```

```python
import jax
import jax.numpy as jnp
from jax import lax
from jax.sharding import PartitionSpec as P

LEN = 128
QLEN = 32
CHUNKS = 2
F32, BF16 = jnp.float32, jnp.bfloat16


X, YL, C, YH, Z = 4, 2, 2, 2, 8
MP = [(x, y, c) for x in range(X) for y in range(YL) for c in range(C)]
DP = [(y, z) for y in range(YH) for z in range(Z)]


def mp_at(x, y, c):
    return (x % X) * 4 + (y % YL) * 2 + c % C


def dp_at(y, z):
    return (y % YH) * Z + z % Z


def move_x(v, by):
    return lax.ppermute(v, "mp", [(mp_at(x, y, c), mp_at(x + by, y, c)) for x, y, c in MP])


def swap_yl(v):
    return lax.ppermute(v, "mp", [(mp_at(x, y, c), mp_at(x, y + 1, c)) for x, y, c in MP])


def swap_core(v):
    return lax.ppermute(v, "mp", [(mp_at(x, y, c), mp_at(x, y, c + 1)) for x, y, c in MP])


def move_z(v, by):
    return lax.ppermute(v, "dp", [(dp_at(y, z), dp_at(y, z + by)) for y, z in DP])


def swap_yh(v):
    return lax.ppermute(v, "dp", [(dp_at(y, z), dp_at(y + 1, z)) for y, z in DP])


def at(v, i):
    return lax.dynamic_index_in_dim(v, i, 0, keepdims=False)


def pick(v, dim, first):
    return jnp.where(first, lax.index_in_dim(v, 0, dim, False), lax.index_in_dim(v, 1, dim, False))


def half_added(v, half, extra):
    parts = [v[0], v[1]]
    parts[half] = parts[half] + extra
    return jnp.stack(parts)


def sum_over_x(seg):
    far = seg(2)
    up, down = move_x(far[0], 1), move_x(far[1], -1)
    from_below = move_x(half_added(seg(1), 0, up), 1)
    from_above = move_x(half_added(seg(3), 1, down), -1)
    return seg(0) + from_below + from_above


def split(v):
    high = lax.reduce_precision(v, 8, 7)
    return high.astype(BF16), (v - high).astype(BF16)


def per_device(
    query_inputs,
    query_grads,
    basis_inputs,
    basis_grads,
    eig_inputs,
    eig_grads,
    train_inputs,
    train_grads,
):
    tokens, feat_in = query_inputs.shape
    feat_out = query_grads.shape[1]
    cols_in, cols_out = basis_inputs.shape[1], basis_grads.shape[1]
    train_count = train_inputs.shape[0]
    rows = tokens // (CHUNKS * len(MP))
    m, d = lax.axis_index("mp"), lax.axis_index("dp")
    my_x, my_yl, my_c = m // 4, (m // 2) % 2, m % 2
    my_yh, my_z = d // Z, d % Z
    eig = jnp.concatenate([eig_inputs, eig_grads])[None, :]
    rot_in = jnp.dot(query_inputs, basis_inputs, preferred_element_type=F32)
    rot_out = jnp.dot(query_grads, basis_grads, preferred_element_type=F32)
    rot_in = rot_in.reshape(X, YL, C, CHUNKS, rows, cols_in)
    rot_out = rot_out.reshape(X, YL, C, CHUNKS, rows, cols_out)

    def rotated(k, first):
        return jnp.concatenate([pick(v[:, :, :, k], 2, first) for v in (rot_in, rot_out)], axis=-1)

    def rotated_and_scaled(k):
        mine = rotated(k, my_c == 0) + swap_core(rotated(k, my_c == 1))
        total = sum_over_x(lambda r: at(mine, (my_x + r) % X))
        final = at(total, my_yl) + swap_yl(at(total, 1 - my_yl))
        return (final / eig).astype(BF16)

    def everyones(own):
        pair = jnp.stack([own, swap_yl(own)])
        below, above = move_x(pair, 1), move_x(pair, -1)
        far = jnp.stack([move_x(below[0], 1), move_x(above[1], -1)])
        mine = jnp.stack([pair, above, far, below])
        return mine, swap_core(mine)

    def back(own):
        flat = jnp.stack(everyones(own)).reshape(-1, cols_in + cols_out)
        v_in = jnp.einsum("qc,fc->qf", flat[:, :cols_in], basis_inputs, preferred_element_type=F32)
        v_out = jnp.einsum("qc,fc->qf", flat[:, cols_in:], basis_grads, preferred_element_type=F32)
        return v_in.reshape(Z, YH, rows, feat_in), v_out.reshape(Z, YH, rows, feat_out)

    def pack(v_in, v_out):
        high, low = split(v_out)
        return jnp.concatenate([v_in.astype(BF16), high, low], axis=-1)

    def unpack(v):
        v_in, high, low = jnp.split(v, [feat_in, feat_in + feat_out], axis=-1)
        return v_in.astype(F32), high.astype(F32) + low.astype(F32)

    def summed_over_dp(v_in, v_out):
        def chain(half, by):
            def seg(r):
                i = (my_z + by * r) % Z
                return at(v_in, i), at(v_out, i)

            s_in, s_out = seg(4)
            r_in, r_out = unpack(move_z(pack(s_in[half], s_out[half]), by))
            s_in, s_out = seg(3)
            got = move_z(pack(half_added(s_in, half, r_in), half_added(s_out, half, r_out)), by)
            for r in (2, 1):
                s_in, s_out = seg(r)
                r_in, r_out = unpack(got)
                got = move_z(pack(s_in + r_in, s_out + r_out), by)
            return unpack(got)

        up_in, up_out = chain(0, 1)
        down_in, down_out = chain(1, -1)
        total = jnp.concatenate(
            [at(v_in, my_z) + up_in + down_in, at(v_out, my_z) + up_out + down_out], axis=-1
        )
        return (at(total, my_yh) + swap_yh(at(total, 1 - my_yh))).astype(BF16)

    def gathered_over_dp(own):
        other = swap_yh(own)
        pair = jnp.where(my_yh == 0, jnp.stack([own, other]), jnp.stack([other, own]))
        whole = jnp.zeros((Z, *pair.shape), BF16)

        def put(whole, v, r):
            return lax.dynamic_update_index_in_dim(whole, v, (my_z + r) % Z, 0)

        whole = put(whole, pair, 0)
        up, down = pair, pair
        for r in (1, 2, 3):
            up, down = move_z(up, 1), move_z(down, -1)
            whole = put(put(whole, up, -r), down, r)
        return put(whole, jnp.stack([move_z(up[0], 1), move_z(down[1], -1)]), 4)

    def scores_of(directions):
        parts = directions.reshape(C, X * YL * rows, feat_in + feat_out)

        def inner(core):
            v_in = jnp.einsum("qf,tf->qt", parts[core, :, :feat_in], train_inputs, preferred_element_type=F32)
            v_out = jnp.einsum("qf,tf->qt", parts[core, :, feat_in:], train_grads, preferred_element_type=F32)
            return jnp.concatenate([v_in, v_out], axis=1).reshape(X, YL, rows, 2 * train_count)

        other = swap_core(inner(1))
        mine = inner(0) + other
        total = sum_over_x(lambda r: mine[r])
        final = total[0] + swap_yl(total[1])
        products = final[:, :train_count] * final[:, train_count:]
        return jnp.sum(products.reshape(rows, train_count // LEN, LEN), axis=(0, 2))

    result = 0.0
    for k in range(CHUNKS):
        own = rotated_and_scaled(k)
        own = summed_over_dp(*back(own))
        result = result + scores_of(gathered_over_dp(own))
    return result[None, :]


def solution(mesh):
    return jax.shard_map(
        per_device,
        mesh=mesh,
        in_specs=(
            P(None, "mp"),
            P(None, "mp"),
            P("mp", "dp"),
            P("mp", "dp"),
            P("dp"),
            P("dp"),
            P("dp", "mp"),
            P("dp", "mp"),
        ),
        out_specs=P("mp", "dp"),
        check_vma=False,
    )
```

```python
import jax
import jax.numpy as jnp
from jax import lax
from jax.sharding import PartitionSpec as P

LEN = 128
QLEN = 32
CHUNKS = 2
F32, BF16 = jnp.float32, jnp.bfloat16


X, YL, C, YH, Z = 4, 2, 2, 2, 8
MP = [(x, y, c) for x in range(X) for y in range(YL) for c in range(C)]
DP = [(y, z) for y in range(YH) for z in range(Z)]


def mp_at(x, y, c):
    return (x % X) * 4 + (y % YL) * 2 + c % C


def dp_at(y, z):
    return (y % YH) * Z + z % Z


def move_x(v, by):
    return lax.ppermute(v, "mp", [(mp_at(x, y, c), mp_at(x + by, y, c)) for x, y, c in MP])


def swap_yl(v):
    return lax.ppermute(v, "mp", [(mp_at(x, y, c), mp_at(x, y + 1, c)) for x, y, c in MP])


def swap_core(v):
    return lax.ppermute(v, "mp", [(mp_at(x, y, c), mp_at(x, y, c + 1)) for x, y, c in MP])


def move_z(v, by):
    return lax.ppermute(v, "dp", [(dp_at(y, z), dp_at(y, z + by)) for y, z in DP])


def swap_yh(v):
    return lax.ppermute(v, "dp", [(dp_at(y, z), dp_at(y + 1, z)) for y, z in DP])


def at(v, i):
    return lax.dynamic_index_in_dim(v, i, 0, keepdims=False)


def pick(v, dim, first):
    return jnp.where(first, lax.index_in_dim(v, 0, dim, False), lax.index_in_dim(v, 1, dim, False))


def half_added(v, half, extra):
    parts = [v[0], v[1]]
    parts[half] = parts[half] + extra
    return jnp.stack(parts)


def sum_over_x(seg):
    far = seg(2)
    up, down = move_x(far[0], 1), move_x(far[1], -1)
    from_below = move_x(half_added(seg(1), 0, up), 1)
    from_above = move_x(half_added(seg(3), 1, down), -1)
    return seg(0) + from_below + from_above


def split(v):
    high = lax.reduce_precision(v, 8, 7)
    return high.astype(BF16), (v - high).astype(BF16)


def per_device(
    query_inputs,
    query_grads,
    basis_inputs,
    basis_grads,
    eig_inputs,
    eig_grads,
    train_inputs,
    train_grads,
):
    tokens, feat_in = query_inputs.shape
    feat_out = query_grads.shape[1]
    cols_in, cols_out = basis_inputs.shape[1], basis_grads.shape[1]
    train_count = train_inputs.shape[0]
    rows = tokens // (CHUNKS * len(MP))
    m, d = lax.axis_index("mp"), lax.axis_index("dp")
    my_x, my_yl, my_c = m // 4, (m // 2) % 2, m % 2
    my_yh, my_z = d // Z, d % Z
    eig = jnp.concatenate([eig_inputs, eig_grads])[None, :]
    rot_in = jnp.dot(query_inputs, basis_inputs, preferred_element_type=F32)
    rot_out = jnp.dot(query_grads, basis_grads, preferred_element_type=F32)
    rot_in = rot_in.reshape(X, YL, C, CHUNKS, rows, cols_in)
    rot_out = rot_out.reshape(X, YL, C, CHUNKS, rows, cols_out)

    def rotated(k, first):
        return jnp.concatenate([pick(v[:, :, :, k], 2, first) for v in (rot_in, rot_out)], axis=-1)

    def rotated_and_scaled(k):
        mine = rotated(k, my_c == 0) + swap_core(rotated(k, my_c == 1))
        total = sum_over_x(lambda r: at(mine, (my_x + r) % X))
        final = pick(total, 0, my_yl == 0) + swap_yl(pick(total, 0, my_yl == 1))
        return (final / eig).astype(BF16)

    def everyones(own):
        pair = jnp.stack([own, swap_yl(own)])
        below, above = move_x(pair, 1), move_x(pair, -1)
        far = jnp.stack([move_x(below[0], 1), move_x(above[1], -1)])
        mine = jnp.stack([pair, above, far, below])
        return mine, swap_core(mine)

    def back(own):
        flat = jnp.stack(everyones(own)).reshape(-1, cols_in + cols_out)
        v_in = jnp.einsum("qc,fc->qf", flat[:, :cols_in], basis_inputs, preferred_element_type=F32)
        v_out = jnp.einsum("qc,fc->qf", flat[:, cols_in:], basis_grads, preferred_element_type=F32)
        return v_in.reshape(Z, YH, rows, feat_in), v_out.reshape(Z, YH, rows, feat_out)

    def pack(v_in, v_out):
        high, low = split(v_out)
        return jnp.concatenate([v_in.astype(BF16), high, low], axis=-1)

    def unpack(v):
        v_in, high, low = jnp.split(v, [feat_in, feat_in + feat_out], axis=-1)
        return v_in.astype(F32), high.astype(F32) + low.astype(F32)

    def summed_over_dp(v_in, v_out):
        def chain(half, by):
            def seg(r):
                i = (my_z + by * r) % Z
                return at(v_in, i), at(v_out, i)

            s_in, s_out = seg(4)
            r_in, r_out = unpack(move_z(pack(s_in[half], s_out[half]), by))
            s_in, s_out = seg(3)
            got = move_z(pack(half_added(s_in, half, r_in), half_added(s_out, half, r_out)), by)
            for r in (2, 1):
                s_in, s_out = seg(r)
                r_in, r_out = unpack(got)
                got = move_z(pack(s_in + r_in, s_out + r_out), by)
            return unpack(got)

        up_in, up_out = chain(0, 1)
        down_in, down_out = chain(1, -1)
        total = jnp.concatenate(
            [at(v_in, my_z) + up_in + down_in, at(v_out, my_z) + up_out + down_out], axis=-1
        )
        return (pick(total, 0, my_yh == 0) + swap_yh(pick(total, 0, my_yh == 1))).astype(BF16)

    def gathered_over_dp(own):
        other = swap_yh(own)
        pair = jnp.where(my_yh == 0, jnp.stack([own, other]), jnp.stack([other, own]))
        whole = jnp.zeros((Z, *pair.shape), BF16)

        def put(whole, v, r):
            return lax.dynamic_update_index_in_dim(whole, v, (my_z + r) % Z, 0)

        whole = put(whole, pair, 0)
        up, down = pair, pair
        for r in (1, 2, 3):
            up, down = move_z(up, 1), move_z(down, -1)
            whole = put(put(whole, up, -r), down, r)
        return put(whole, jnp.stack([move_z(up[0], 1), move_z(down[1], -1)]), 4)

    def scores_of(directions):
        parts = directions.reshape(C, X * YL * rows, feat_in + feat_out)

        def inner(core):
            v_in = jnp.einsum("qf,tf->qt", parts[core, :, :feat_in], train_inputs, preferred_element_type=F32)
            v_out = jnp.einsum("qf,tf->qt", parts[core, :, feat_in:], train_grads, preferred_element_type=F32)
            return jnp.concatenate([v_in, v_out], axis=1).reshape(X, YL, rows, 2 * train_count)

        other = swap_core(inner(1))
        mine = inner(0) + other
        total = sum_over_x(lambda r: mine[r])
        final = total[0] + swap_yl(total[1])
        products = final[:, :train_count] * final[:, train_count:]
        return jnp.sum(products.reshape(rows, train_count // LEN, LEN), axis=(0, 2))

    result = 0.0
    for k in range(CHUNKS):
        own = rotated_and_scaled(k)
        own = summed_over_dp(*back(own))
        result = result + scores_of(gathered_over_dp(own))
    return result[None, :]


def solution(mesh):
    return jax.shard_map(
        per_device,
        mesh=mesh,
        in_specs=(
            P(None, "mp"),
            P(None, "mp"),
            P("mp", "dp"),
            P("mp", "dp"),
            P("dp"),
            P("dp"),
            P("dp", "mp"),
            P("dp", "mp"),
        ),
        out_specs=P("mp", "dp"),
        check_vma=False,
    )
```
